32 devices in a mesh: gz: 16 (over z, y, x), ta: 2 (over core).
Axes of the slice: x: 2, y: 2, z: 4, core: 2. Of those that a mesh axis runs over, the one named last changes fastest.
Arguments:
- position: float32 [2, 48, 32, 512], P(None, 'gz', 'ta'), may hold values from -6 to 6
- gaps: float32 [2, 3, 48, 32, 512], P(None, None, 'gz', 'ta'), may hold values from -6 to 6
- weights: float32 [3, 48, 32, 512], P(None, 'gz', 'ta'), may hold values from 0.2 to 2
- deltas: int32 [3, 48, 32, 512], P(None, 'gz', 'ta'), may hold values from 0 to 8
- springs: int32 [2, 48, 32, 512], P(None, 'gz', 'ta'), may hold values 0 or 1
- damping: float32 [48, 32, 512], P('gz', 'ta'), may hold values from 0.1 to 1
- stiffness: float32 [2, 48], P(None, 'gz'), may hold values from 0.5 to 4
Outputs:
- update: float32 [2, 48, 32, 512], P(None, 'gz', 'ta')
- residual: float32 [2, 48, 32, 512], P(None, 'gz', 'ta')
The draws below stay inside these ranges and needn't reach their ends.
All inputs are finite; a program needn't handle non-finite values. No bound on the sum of `springs` on one device may be relied on, other than what follows from the above.
Results may differ from the reference program's by a relative error of at most 0.00012.
Values sent between devices are 32-bit elements; how exact they have to be, the bound alone decides.
A program may use at most 64 MiB of HBM per device.

```python
import math
import jax
import jax.numpy as jnp
from jax import lax

COLS = 512
ITERS = 2
SECTIONS = 48
ROWS = 32


def touch_ends(entries, key, least, high):
    longest = entries.shape.index(max(entries.shape))
    spots = []
    for shift in (0, 1):
        where = [jax.random.randint(jax.random.fold_in(key, axis), (), 0, length) for axis, length in enumerate(entries.shape)]
        where[longest] = (where[longest] + shift) % entries.shape[longest]
        spots.append(tuple(where))
    return entries.at[spots[0]].set(least).at[spots[1]].set(high)


def shard_levels(rng, dims, pieces, low, largest):
    def one(axis_at, blocks):
        steps = jax.random.uniform(jax.random.fold_in(jax.random.fold_in(rng, 6), axis_at), (blocks,), jnp.float32, low / len(pieces), largest / len(pieces))
        return jnp.repeat(jnp.exp(steps), dims[axis_at] // blocks).reshape((-1,) + (1,) * (len(dims) - axis_at - 1))

    loudness = one(*pieces[0])
    for cut in pieces[1:]:
        loudness = loudness * one(*cut)
    return loudness


def centred(stream_key, dims, width, most, pieces=(), kind=jnp.bfloat16):
    array = width * jax.random.normal(stream_key, dims, jnp.float32)
    if pieces:
        array = array * shard_levels(stream_key, dims, pieces, -0.22, 0.18)
    return jnp.clip(array, -most, most).astype(kind)


def setup_inputs(seed: int = 0) -> dict:
    streams_of = jax.random.split(jax.random.key(seed), 8)
    return {
        "position": centred(streams_of[0], (2, SECTIONS, ROWS, COLS), 1.0, 6.0, ((1, 16), (2, 2)), jnp.float32),
        "gaps": centred(streams_of[1], (2, 3, SECTIONS, ROWS, COLS), 1.0, 6.0, ((2, 16), (3, 2)), jnp.float32),
        "weights": jnp.clip(jnp.exp(math.log(2.0) - 2.3025851 * jax.random.uniform(streams_of[2], (3, SECTIONS, ROWS, COLS), jnp.float32) ** shard_levels(streams_of[2], (3, SECTIONS, ROWS, COLS), ((1, 16), (2, 2)), -0.2, 0.2)), 0.2, 2.0),
        "deltas": touch_ends(jax.random.randint(streams_of[3], (3, SECTIONS, ROWS, COLS), 0, 9), jax.random.fold_in(streams_of[3], 1), 0, 8).astype(jnp.int32),
        "springs": touch_ends((jax.random.randint(streams_of[4], (2, SECTIONS, ROWS, COLS), 0, 10) < 9).astype(jnp.int32), jax.random.fold_in(streams_of[4], 1), 0, 1),
        "damping": jnp.clip(jnp.exp(math.log(1.0) - 2.3025851 * jax.random.uniform(streams_of[5], (SECTIONS, ROWS, COLS), jnp.float32) ** shard_levels(streams_of[5], (SECTIONS, ROWS, COLS), ((0, 16), (1, 2)), -0.2, 0.2)), 0.1, 1.0),
        "stiffness": jnp.clip(jnp.exp(math.log(4.0) - 2.0794415 * jax.random.uniform(streams_of[6], (2, SECTIONS), jnp.float32) ** shard_levels(streams_of[6], (2, SECTIONS), ((1, 16),), -0.2, 0.2)), 0.5, 4.0),
    }


def shift_along(values, axis, step):
    if step == 0:
        return values
    length = values.shape[axis]
    widths = [(0, 0)] * values.ndim
    if step > 0:
        kept = lax.slice_in_dim(values, 0, length - step, axis=axis)
        widths[axis] = (step, 0)
    else:
        kept = lax.slice_in_dim(values, -step, length, axis=axis)
        widths[axis] = (0, -step)
    return jnp.pad(kept, widths)


def take_columns(field, delta):
    columns_at = lax.broadcasted_iota(jnp.int32, delta.shape, 2)
    index = jnp.clip(columns_at + delta - 4, 0, delta.shape[2] - 1).astype(jnp.int32)
    return jnp.take_along_axis(field, jnp.broadcast_to(index, field.shape), axis=3)


def column_valid(delta):
    columns_at = lax.broadcasted_iota(jnp.int32, delta.shape, 2)
    target = columns_at + delta - 4
    return jnp.where((target >= 0) & (target < delta.shape[2]), 1.0, 0.0).astype(jnp.float32)


def put_columns(values, delta):
    total = jnp.zeros_like(values)
    for place in range(9):
        total = total + shift_along(jnp.where(delta == place, values, 0.0), 3, place - 4)
    return total


def operator(field, gap_set, weights, deltas, springs, damping, stiffness):
    count, rows, cols = damping.shape
    sections_at = lax.broadcasted_iota(jnp.int32, (count, rows, cols), 0)
    rows_at = lax.broadcasted_iota(jnp.int32, (count, rows, cols), 1)
    columns_at = lax.broadcasted_iota(jnp.int32, (count, rows, cols), 2)
    along = stiffness[0][:, None, None]
    across = stiffness[1][:, None, None]
    horiz = jnp.where((springs[0] > 0) & (columns_at < cols - 1), 1.0, 0.0).astype(jnp.float32)
    vert = jnp.where((springs[1] > 0) & (rows_at < rows - 1), 1.0, 0.0).astype(jnp.float32)
    h_flux = along * horiz * (shift_along(field, 3, -1) - field)
    v_flux = across * vert * (shift_along(field, 2, -1) - field)
    total = damping * field - h_flux + shift_along(h_flux, 3, 1) - v_flux + shift_along(v_flux, 2, 1)
    for slot in range(3):
        offset = slot + 1
        partner = take_columns(shift_along(field, 1, -offset), deltas[slot])
        inside = jnp.where(sections_at + offset < count, 1.0, 0.0).astype(jnp.float32)
        strength = weights[slot] * column_valid(deltas[slot]) * inside
        mismatch = field - partner
        if gap_set is not None:
            mismatch = mismatch - gap_set[:, slot]
        pulled = strength * mismatch
        total = total + pulled - shift_along(put_columns(pulled, deltas[slot]), 1, offset)
    return total


def reference(position, gaps, weights, deltas, springs, damping, stiffness):
    rhs = -operator(position, gaps, weights, deltas, springs, damping, stiffness)
    update = jnp.zeros_like(rhs)
    residual = rhs
    direction = rhs
    norm_now = jnp.sum(residual * residual)
    for step in range(ITERS):
        image = operator(direction, None, weights, deltas, springs, damping, stiffness)
        alpha = norm_now / jnp.sum(direction * image)
        update = update + alpha * direction
        residual = residual - alpha * image
        norm_next = jnp.sum(residual * residual)
        direction = residual + (norm_next / norm_now) * direction
        norm_now = norm_next
    return update, residual
```

```python
import functools

import jax
import jax.numpy as jnp
from jax import lax
from jax.experimental import pallas as pl
from jax.experimental.pallas import tpu as pltpu
from jax.sharding import PartitionSpec as P

MESH = pl.DeviceIdType.MESH
PLACES = 9
HALF = 8
OPS = 3
LANES = 128
VMEM = 67043328


def rolled(values, step):
    axis = values.ndim - 1
    return values if step == 0 else pltpu.roll(values, step % values.shape[axis], axis)


def doublings(n):
    reach, out = 1, []
    while reach < n:
        out.append(reach)
        reach *= 2
    return out


def kernel(
    n, pos_h, gaps_h, wei_h, del_h, spr_h, dam_h, stiff,
    upd, res,
    pos, r0, m0, up, tsend, trecv, esend, erecv, sall, gath,
    gaps, wei, dlt, spr, dam, vc, va, hc, hl, diag, accb, qbuf, dots,
    load_sem, vs_sem, vr_sem, ts_sem, tr_sem, es_sem, er_sem, gs_sem, gr_sem, reach_sem,
):
    g = lax.axis_index("gz")
    t = lax.axis_index("ta")
    secs, rows, cols = dam_h.shape
    chunks = rows // HALF
    other = {"gz": g, "ta": 1 - t}
    lower = {"gz": g - 1, "ta": t}
    upper = {"gz": g + 1, "ta": t}
    has_lower = g > 0
    has_upper = g < n - 1
    fields = [pos, r0, m0]

    loads = [
        pltpu.make_async_copy(pos_h, pos, load_sem.at[0]),
        pltpu.make_async_copy(spr_h, spr, load_sem.at[1]),
        pltpu.make_async_copy(del_h, dlt, load_sem.at[2]),
        pltpu.make_async_copy(wei_h, wei, load_sem.at[3]),
        pltpu.make_async_copy(dam_h, dam, load_sem.at[4]),
        pltpu.make_async_copy(gaps_h, gaps, load_sem.at[5]),
    ]
    for load in loads:
        load.start()

    barrier = pltpu.get_barrier_semaphore()
    pl.semaphore_signal(barrier, inc=1, device_id=other, device_id_type=MESH)

    @pl.when(has_lower)
    def _():
        pl.semaphore_signal(barrier, inc=1, device_id=lower, device_id_type=MESH)

    @pl.when(has_upper)
    def _():
        pl.semaphore_signal(barrier, inc=1, device_id=upper, device_id_type=MESH)

    @pl.when(jnp.logical_not(has_upper))
    def _():
        up[...] = jnp.zeros_like(up)

    @pl.when(jnp.logical_not(has_lower))
    def _():
        trecv[...] = jnp.zeros_like(trecv)

    esend[...] = jnp.zeros_like(esend)
    dots[...] = jnp.zeros_like(dots)

    def rows_at(h):
        return pl.ds(h * HALF, HALF)

    def v_copy(op, d, h):
        return pltpu.make_async_remote_copy(
            fields[op].at[:, d, rows_at(h)], up.at[op, :, d, rows_at(h)],
            vs_sem.at[op, d * chunks + h], vr_sem.at[op, d * chunks + h], device_id=lower, device_id_type=MESH,
        )

    def t_copy(op, d, h):
        return pltpu.make_async_remote_copy(
            tsend.at[op, :, d, rows_at(h)], trecv.at[op, :, d, rows_at(h)],
            ts_sem.at[op, d * chunks + h], tr_sem.at[op, d * chunks + h], device_id=upper, device_id_type=MESH,
        )

    def e_copy(op):
        return pltpu.make_async_remote_copy(
            esend.at[op], erecv.at[op], es_sem.at[op], er_sem.at[op],
            device_id=other, device_id_type=MESH,
        )

    far = doublings(n)

    def reach_signal(i):
        for sign in (-1, 1):
            there = g + sign * far[i]

            @pl.when((there >= 0) & (there < n))
            def _():
                pl.semaphore_signal(
                    reach_sem.at[i], inc=1, device_id={"gz": there, "ta": t}, device_id_type=MESH
                )

    def reach_wait(i):
        pl.semaphore_wait(
            reach_sem.at[i],
            (g >= far[i]).astype(jnp.int32) + (g + far[i] < n).astype(jnp.int32),
        )

    pending = list(range(len(far)))

    def reach_step():
        if pending:
            i = pending.pop(0)
            reach_wait(i)
            if i + 1 < len(far):
                reach_signal(i + 1)

    def send_edges(op):
        for comp in range(2):
            for z in range(secs):
                k = comp * secs + z
                top = fields[op][comp, z, 0:1, :]
                bottom = fields[op][comp, z, rows - 1 : rows, :]
                esend[op, k : k + 1, :] = jnp.where(t == 0, bottom, top)
        if op == 0:
            for z in range(secs):
                k = 2 * secs + z
                esend[op, k : k + 1, :] = jnp.where(
                    spr[1, z, rows - 1 : rows, :] > 0, 1.0, 0.0
                ).astype(jnp.float32)
        e_copy(op).start()

    shape = (HALF, cols)
    columns_at = lax.broadcasted_iota(jnp.int32, shape, 1)
    row_at = lax.broadcasted_iota(jnp.int32, shape, 0)

    def dot_into(i, a, b):
        dots[i] = dots[i] + (a[0] * b[0] + a[1] * b[1])

    def pulls(op, s, h):
        field = fields[op][:, s, rows_at(h)] if s < secs else up[op, :, s - secs, rows_at(h)]
        sources = [(s - k - 1, k) for k in range(3) if 0 <= s - k - 1 < secs]
        got = [None] * len(sources)
        for place in range(PLACES):
            moved = rolled(field, 4 - place)
            for i, (z, k) in enumerate(sources):
                if got[i] is None:
                    got[i] = moved
                else:
                    got[i] = jnp.where((dlt[k, z, rows_at(h)] == place)[None], moved, got[i])
        out = []
        for i, (z, k) in enumerate(sources):
            miss = fields[op][:, z, rows_at(h)] - got[i]
            if op == 0:
                miss = miss - gaps[:, k, z, rows_at(h)]
            out.append((z, k, miss, wei[k, z, rows_at(h)][None] * miss))
        return out

    def scatter(terms, h):
        total = None
        for place in range(PLACES):
            part = None
            for z, k, _, pulled in terms:
                one = jnp.where((dlt[k, z, rows_at(h)] == place)[None], pulled, 0.0)
                part = one if part is None else part + one
            part = rolled(part, place - 4)
            total = part if total is None else total + part
        return total

    def own(op, h):
        here = rows_at(h)
        acc = []
        for z in range(secs):
            center = fields[op][:, z, here]
            acc.append(
                diag[z, here][None] * center
                - hc[z, here][None] * rolled(center, -1)
                - hl[z, here][None] * rolled(center, 1)
            )
        for s in range(1, secs):
            terms = pulls(op, s, h)
            for z, _, _, pulled in terms:
                acc[z] = acc[z] + pulled
            acc[s] = acc[s] - scatter(terms, h)
        for z in range(secs):
            accb[:, z, here] = acc[z]

    def vertical(op):
        for h in range(chunks):
            here = rows_at(h)
            for z in range(secs):
                for comp in range(2):
                    k = comp * secs + z
                    center = fields[op][comp, z, here]
                    if h == 0:
                        above = jnp.where(row_at == 0, erecv[op, k : k + 1, :], pltpu.roll(center, 1, 0))
                    else:
                        above = fields[op][comp, z, pl.ds(h * HALF - 1, HALF)]
                    if h == chunks - 1:
                        below = jnp.where(
                            row_at == HALF - 1, erecv[op, k : k + 1, :], pltpu.roll(center, HALF - 1, 0)
                        )
                    else:
                        below = fields[op][comp, z, pl.ds(h * HALF + 1, HALF)]
                    accb[comp, z, here] = accb[comp, z, here] - vc[z, here] * below - va[z, here] * above
                if op == OPS - 1:
                    dot_into(3, fields[op][:, z, here], accb[:, z, here])

    def cross(op, d, h):
        @pl.when(has_upper)
        def _():
            v_copy(op, d, h).wait_recv()

        terms = pulls(op, secs + d, h)
        tsend[op, :, d, rows_at(h)] = scatter(terms, h)

        @pl.when(has_upper)
        def _():
            t_copy(op, d, h).start()

        for z, _, miss, pulled in terms:
            accb[:, z, rows_at(h)] = accb[:, z, rows_at(h)] + pulled
            if op == OPS - 1:
                dot_into(3, miss, pulled)

    def finish(op, z, h):
        here = rows_at(h)

        @pl.when(has_lower)
        def _():
            t_copy(op, z, h).wait_recv()

        image = accb[:, z, here] - trecv[op, :, z, here]
        if op == 0:
            r0[:, z, here] = -image
        elif op == 1:
            m0[:, z, here] = image
        else:
            qbuf[:, z, here] = image
        if op + 1 < OPS:
            @pl.when(has_lower)
            def _():
                v_copy(op + 1, z, h).start()
        if op == 0:
            dot_into(0, image, image)
        elif op == 1:
            dot_into(1, r0[:, z, here], image)
            dot_into(2, image, image)

    pieces = [(d, h) for d in range(secs) for h in range(chunks)]

    loads[0].wait()
    pl.semaphore_wait(barrier, 1 + has_lower.astype(jnp.int32) + has_upper.astype(jnp.int32))

    @pl.when(has_lower)
    def _():
        for d, h in pieces:
            v_copy(0, d, h).start()

    loads[1].wait()
    send_edges(0)
    if far:
        reach_signal(0)
    loads[2].wait()
    loads[3].wait()
    for k in range(3):
        for z in range(secs):
            inside = jnp.where(g * secs + z + k + 1 < n * secs, 1.0, 0.0).astype(jnp.float32)
            for h in range(chunks):
                target = columns_at + dlt[k, z, rows_at(h)] - 4
                valid = (target >= 0) & (target < cols)
                wei[k, z, rows_at(h)] = jnp.where(valid, wei[k, z, rows_at(h)], 0.0) * inside
    loads[4].wait()
    for z in range(secs):
        for h in range(chunks):
            last = jnp.where((t == 1) & (row_at == HALF - 1), 0.0, 1.0) if h == chunks - 1 else 1.0
            vc[z, rows_at(h)] = (
                stiff[1, z] * jnp.where(spr[1, z, rows_at(h)] > 0, 1.0, 0.0).astype(jnp.float32) * last
            )
            right = stiff[0, z] * jnp.where(
                (spr[0, z, rows_at(h)] > 0) & (columns_at < cols - 1), 1.0, 0.0
            ).astype(jnp.float32)
            hc[z, rows_at(h)] = right
            left = rolled(right, 1)
            hl[z, rows_at(h)] = left
            diag[z, rows_at(h)] = dam[z, rows_at(h)] + right + left
    e_copy(0).wait_recv()
    for z in range(secs):
        k = 2 * secs + z
        edge = jnp.where(t == 1, stiff[1, z] * erecv[0, k : k + 1, :], 0.0)
        for h in range(chunks):
            if h == 0:
                above = jnp.where(row_at == 0, edge, pltpu.roll(vc[z, rows_at(h)], 1, 0))
            else:
                above = vc[z, pl.ds(h * HALF - 1, HALF)]
            va[z, rows_at(h)] = above
            diag[z, rows_at(h)] = diag[z, rows_at(h)] + vc[z, rows_at(h)] + above
    loads[5].wait()

    def reduce_start():
        packed = jnp.zeros((8, LANES), jnp.float32)
        sub = lax.broadcasted_iota(jnp.int32, (8, LANES), 0)
        for i in range(4):
            row = jnp.sum(dots[i], axis=0, keepdims=True)
            part = row[:, 0:LANES]
            for c in range(LANES, cols, LANES):
                part = part + row[:, c : c + LANES]
            packed = jnp.where(sub == i, part, packed)
        esend[OPS, 0:8, 0:LANES] = packed
        e_copy(OPS).start()
        e_copy(OPS).wait_recv()
        sall[...] = packed + erecv[OPS, 0:8, 0:LANES]
        pushes = []
        for j in range(1, n):
            pushes.append(
                pltpu.make_async_remote_copy(
                    sall, gath.at[j - 1], gs_sem.at[j - 1], gr_sem.at[j - 1],
                    device_id={"gz": lax.rem(g + j, n), "ta": t}, device_id_type=MESH,
                )
            )
        for push in pushes:
            push.start()
        return pushes

    for op in range(OPS):
        for h in range(chunks):
            own(op, h)
        if op > 0:
            e_copy(op).wait_recv()
        vertical(op)
        reach_step()
        for d, h in pieces:
            cross(op, d, h)
        if op == OPS - 1:
            while pending:
                reach_step()
            pushes = reduce_start()
        else:
            reach_step()
        for z, h in pieces:
            finish(op, z, h)
        if op + 1 < OPS:
            send_edges(op + 1)

    for push in pushes:
        push.wait_recv()
    total = sall[...]
    for j in range(1, n):
        total = total + gath[j - 1]
    total = jnp.sum(total, axis=1, keepdims=True)
    rr, rm, mm, mq = (total[i : i + 1, :] for i in range(4))
    alpha0 = rr / rm
    rr1 = alpha0 * (alpha0 * mm) - rr
    ratio = rr1 / rr
    one = 1.0 + ratio
    curve = one * one * rm - 2.0 * one * alpha0 * mm + alpha0 * alpha0 * mq
    alpha1 = rr1 / curve
    c1 = alpha0 + alpha1 * one
    c2 = alpha0 * alpha1
    for z in range(secs):
        for h in range(chunks):
            here = rows_at(h)
            for comp in range(2):
                a = r0[comp, z, here]
                b = m0[comp, z, here]
                upd[comp, z, here] = c1 * a - c2 * b
                res[comp, z, here] = a - c1 * b + c2 * qbuf[comp, z, here]

    for push in pushes:
        push.wait_send()
    for op in range(OPS + 1):
        e_copy(op).wait_send()

    @pl.when(has_lower)
    def _():
        for op in range(OPS):
            for d, h in pieces:
                v_copy(op, d, h).wait_send()

    @pl.when(has_upper)
    def _():
        for op in range(OPS):
            for d, h in pieces:
                t_copy(op, d, h).wait_send()


def body(position, gaps, weights, deltas, springs, damping, stiffness):
    secs, rows, cols = damping.shape
    n = lax.axis_size("gz")
    chunks = rows // HALF
    f32, i32 = jnp.float32, jnp.int32
    edge = -(-3 * secs // 8) * 8
    dma = pltpu.SemaphoreType.DMA
    out = pltpu.VMEM(position.shape, f32)
    anyspace = pl.BlockSpec(memory_space=pl.ANY)
    vmem = pl.BlockSpec(memory_space=pltpu.VMEM)
    field = pltpu.VMEM(position.shape, f32)
    plane = pltpu.VMEM(damping.shape, f32)
    exchange = pltpu.VMEM((OPS,) + position.shape, f32)
    piece_sems = dma((OPS, secs * chunks))
    return pl.pallas_call(
        functools.partial(kernel, n),
        out_shape=(out, out),
        in_specs=[anyspace] * 6 + [pl.BlockSpec(memory_space=pltpu.SMEM)],
        out_specs=(vmem, vmem),
        scratch_shapes=[
            field, field, field,
            exchange, exchange, exchange,
            pltpu.VMEM((OPS + 1, edge, cols), f32),
            pltpu.VMEM((OPS + 1, edge, cols), f32),
            pltpu.VMEM((8, LANES), f32),
            pltpu.VMEM((n - 1, 8, LANES), f32),
            pltpu.VMEM(gaps.shape, f32),
            pltpu.VMEM(weights.shape, f32),
            pltpu.VMEM(deltas.shape, i32),
            pltpu.VMEM(springs.shape, i32),
            plane, plane, plane, plane, plane, plane,
            field, field,
            pltpu.VMEM((4, HALF, cols), f32),
            dma((6,)),
            piece_sems, piece_sems, piece_sems, piece_sems,
            dma((OPS + 1,)), dma((OPS + 1,)),
            dma((n - 1,)), dma((n - 1,)),
            pltpu.SemaphoreType.REGULAR((max(len(doublings(n)), 1),)),
        ],
        compiler_params=pltpu.CompilerParams(
            collective_id=0, has_side_effects=True, vmem_limit_bytes=VMEM - 2 * 4 * position.size
        ),
    )(*[pltpu.with_memory_space_constraint(x, pltpu.HBM) for x in (position, gaps, weights, deltas, springs, damping)], stiffness)


def solution(mesh):
    return jax.shard_map(
        body,
        mesh=mesh,
        in_specs=(
            P(None, "gz", "ta", None),
            P(None, None, "gz", "ta", None),
            P(None, "gz", "ta", None),
            P(None, "gz", "ta", None),
            P(None, "gz", "ta", None),
            P("gz", "ta", None),
            P(None, "gz"),
        ),
        out_specs=(P(None, "gz", "ta", None), P(None, "gz", "ta", None)),
        check_vma=False,
    )
```

```python
import functools

import jax
import jax.numpy as jnp
from jax import lax
from jax.experimental import pallas as pl
from jax.experimental.pallas import tpu as pltpu
from jax.sharding import PartitionSpec as P

MESH = pl.DeviceIdType.MESH
PLACES = 9
HALF = 8
OPS = 3
LANES = 128
VMEM = 67043328


def rolled(values, step):
    axis = values.ndim - 1
    return values if step == 0 else pltpu.roll(values, step % values.shape[axis], axis)


def doublings(n):
    reach, out = 1, []
    while reach < n:
        out.append(reach)
        reach *= 2
    return out


def kernel(
    n, pos_h, gaps_h, wei_h, del_h, spr_h, dam_h, stiff_h,
    r0, m0, qbuf, coef,
    stiff, pos, up, tsend, trecv, esend, erecv, sall, gath,
    gaps, wei, dlt, spr, dam, vc, va, hc, hl, diag, accb, dots,
    load_sem, vs_sem, vr_sem, ts_sem, tr_sem, es_sem, er_sem, gs_sem, gr_sem, reach_sem,
):
    g = lax.axis_index("gz")
    t = lax.axis_index("ta")
    secs, rows, cols = dam_h.shape
    chunks = rows // HALF
    other = {"gz": g, "ta": 1 - t}
    lower = {"gz": g - 1, "ta": t}
    upper = {"gz": g + 1, "ta": t}
    has_lower = g > 0
    has_upper = g < n - 1
    fields = [pos, r0, m0]

    loads = [
        pltpu.make_async_copy(pos_h, pos, load_sem.at[0]),
        pltpu.make_async_copy(spr_h, spr, load_sem.at[1]),
        pltpu.make_async_copy(del_h, dlt, load_sem.at[2]),
        pltpu.make_async_copy(wei_h, wei, load_sem.at[3]),
        pltpu.make_async_copy(dam_h, dam, load_sem.at[4]),
        pltpu.make_async_copy(gaps_h, gaps, load_sem.at[5]),
        pltpu.make_async_copy(stiff_h, stiff, load_sem.at[6]),
    ]
    for load in loads:
        load.start()

    barrier = pltpu.get_barrier_semaphore()
    pl.semaphore_signal(barrier, inc=1, device_id=other, device_id_type=MESH)

    @pl.when(has_lower)
    def _():
        pl.semaphore_signal(barrier, inc=1, device_id=lower, device_id_type=MESH)

    @pl.when(has_upper)
    def _():
        pl.semaphore_signal(barrier, inc=1, device_id=upper, device_id_type=MESH)

    @pl.when(jnp.logical_not(has_upper))
    def _():
        up[...] = jnp.zeros_like(up)

    @pl.when(jnp.logical_not(has_lower))
    def _():
        trecv[...] = jnp.zeros_like(trecv)

    esend[...] = jnp.zeros_like(esend)
    dots[...] = jnp.zeros_like(dots)

    def rows_at(h):
        return pl.ds(h * HALF, HALF)

    def v_copy(op, d, h):
        return pltpu.make_async_remote_copy(
            fields[op].at[:, d, rows_at(h)], up.at[op, :, d, rows_at(h)],
            vs_sem.at[0], vr_sem.at[d * chunks + h], device_id=lower, device_id_type=MESH,
        )

    def t_copy(op, d, h):
        return pltpu.make_async_remote_copy(
            tsend.at[op, :, d, rows_at(h)], trecv.at[op, :, d, rows_at(h)],
            ts_sem.at[0], tr_sem.at[d * chunks + h], device_id=upper, device_id_type=MESH,
        )

    def e_copy(op):
        return pltpu.make_async_remote_copy(
            esend.at[op], erecv.at[op], es_sem.at[0], er_sem.at[op],
            device_id=other, device_id_type=MESH,
        )

    far = doublings(n)

    def reach_signal(i):
        for sign in (-1, 1):
            there = g + sign * far[i]

            @pl.when((there >= 0) & (there < n))
            def _():
                pl.semaphore_signal(
                    reach_sem.at[i], inc=1, device_id={"gz": there, "ta": t}, device_id_type=MESH
                )

    def reach_wait(i):
        pl.semaphore_wait(
            reach_sem.at[i],
            (g >= far[i]).astype(jnp.int32) + (g + far[i] < n).astype(jnp.int32),
        )

    pending = list(range(len(far)))

    def reach_step():
        if pending:
            i = pending.pop(0)
            reach_wait(i)
            if i + 1 < len(far):
                reach_signal(i + 1)

    def send_edges(op):
        for comp in range(2):
            for z in range(secs):
                k = comp * secs + z
                top = fields[op][comp, z, 0:1, :]
                bottom = fields[op][comp, z, rows - 1 : rows, :]
                esend[op, k : k + 1, :] = jnp.where(t == 0, bottom, top)
        if op == 0:
            for z in range(secs):
                k = 2 * secs + z
                esend[op, k : k + 1, :] = jnp.where(
                    spr[1, z, rows - 1 : rows, :] > 0, 1.0, 0.0
                ).astype(jnp.float32)
        e_copy(op).start()

    shape = (HALF, cols)
    columns_at = lax.broadcasted_iota(jnp.int32, shape, 1)
    row_at = lax.broadcasted_iota(jnp.int32, shape, 0)

    def dot_into(i, a, b):
        dots[i] = dots[i] + (a[0] * b[0] + a[1] * b[1])

    def pulls(op, s, h):
        field = fields[op][:, s, rows_at(h)] if s < secs else up[op, :, s - secs, rows_at(h)]
        sources = [(s - k - 1, k) for k in range(3) if 0 <= s - k - 1 < secs]
        got = [None] * len(sources)
        for place in range(PLACES):
            moved = rolled(field, 4 - place)
            for i, (z, k) in enumerate(sources):
                if got[i] is None:
                    got[i] = moved
                else:
                    got[i] = jnp.where((dlt[k, z, rows_at(h)] == place)[None], moved, got[i])
        out = []
        for i, (z, k) in enumerate(sources):
            miss = fields[op][:, z, rows_at(h)] - got[i]
            if op == 0:
                miss = miss - gaps[:, k, z, rows_at(h)]
            out.append((z, k, got[i], miss, wei[k, z, rows_at(h)][None] * miss))
        return out

    def scatter(terms, h):
        total = None
        for place in range(PLACES):
            part = None
            for z, k, _, _, pulled in terms:
                one = jnp.where((dlt[k, z, rows_at(h)] == place)[None], pulled, 0.0)
                part = one if part is None else part + one
            part = rolled(part, place - 4)
            total = part if total is None else total + part
        return total

    def own_pairs(op, s, h):
        here = rows_at(h)
        terms = pulls(op, s, h)
        for z, _, _, _, pulled in terms:
            accb[:, z, here] = accb[:, z, here] + pulled
        accb[:, s, here] = accb[:, s, here] - scatter(terms, h)

    def own_springs(op, h):
        here = rows_at(h)
        for z in range(secs):
            for comp in range(2):
                k = comp * secs + z
                center = fields[op][comp, z, here]
                if h == 0:
                    above = jnp.where(row_at == 0, erecv[op, k : k + 1, :], pltpu.roll(center, 1, 0))
                else:
                    above = fields[op][comp, z, pl.ds(h * HALF - 1, HALF)]
                if h == chunks - 1:
                    below = jnp.where(
                        row_at == HALF - 1, erecv[op, k : k + 1, :], pltpu.roll(center, HALF - 1, 0)
                    )
                else:
                    below = fields[op][comp, z, pl.ds(h * HALF + 1, HALF)]
                accb[comp, z, here] = (
                    accb[comp, z, here]
                    + diag[z, here] * center
                    - hc[z, here] * rolled(center, -1)
                    - hl[z, here] * rolled(center, 1)
                    - vc[z, here] * below
                    - va[z, here] * above
                )
            if op == OPS - 1:
                dot_into(3, fields[op][:, z, here], accb[:, z, here])

    def cross(op, d, h):
        @pl.when(has_upper)
        def _():
            v_copy(op, d, h).wait_recv()

        terms = pulls(op, secs + d, h)
        tsend[op, :, d, rows_at(h)] = scatter(terms, h)

        @pl.when(has_upper)
        def _():
            t_copy(op, d, h).start()

        started = d == 0
        for z, _, partner, _, pulled in terms:
            before = 0.0 if started else accb[:, z, rows_at(h)]
            accb[:, z, rows_at(h)] = before + pulled
            if op == OPS - 1:
                dot_into(3, -partner, pulled)

    def finish(op, z, h):
        here = rows_at(h)

        @pl.when(has_lower)
        def _():
            t_copy(op, z, h).wait_recv()

        image = accb[:, z, here] - trecv[op, :, z, here]
        if op == 0:
            r0[:, z, here] = -image
        elif op == 1:
            m0[:, z, here] = image
        else:
            qbuf[:, z, here] = image
        if op + 1 < OPS:
            @pl.when(has_lower)
            def _():
                v_copy(op + 1, z, h).start()
        if op == 0:
            dot_into(0, image, image)
        elif op == 1:
            dot_into(1, r0[:, z, here], image)
            dot_into(2, image, image)

    pieces = [(d, h) for d in range(secs) for h in range(chunks)]

    loads[0].wait()
    pl.semaphore_wait(barrier, 1 + has_lower.astype(jnp.int32) + has_upper.astype(jnp.int32))

    @pl.when(has_lower)
    def _():
        for d, h in pieces:
            v_copy(0, d, h).start()

    loads[1].wait()
    send_edges(0)
    if far:
        reach_signal(0)
    loads[2].wait()
    loads[3].wait()
    for k in range(3):
        for z in range(secs):
            inside = jnp.where(g * secs + z + k + 1 < n * secs, 1.0, 0.0).astype(jnp.float32)
            for h in range(chunks):
                target = columns_at + dlt[k, z, rows_at(h)] - 4
                valid = (target >= 0) & (target < cols)
                wei[k, z, rows_at(h)] = jnp.where(valid, wei[k, z, rows_at(h)], 0.0) * inside
    loads[4].wait()
    loads[6].wait()
    for z in range(secs):
        for h in range(chunks):
            last = jnp.where((t == 1) & (row_at == HALF - 1), 0.0, 1.0) if h == chunks - 1 else 1.0
            vc[z, rows_at(h)] = (
                stiff[1, z] * jnp.where(spr[1, z, rows_at(h)] > 0, 1.0, 0.0).astype(jnp.float32) * last
            )
            right = stiff[0, z] * jnp.where(
                (spr[0, z, rows_at(h)] > 0) & (columns_at < cols - 1), 1.0, 0.0
            ).astype(jnp.float32)
            hc[z, rows_at(h)] = right
            left = rolled(right, 1)
            hl[z, rows_at(h)] = left
            diag[z, rows_at(h)] = dam[z, rows_at(h)] + right + left
    e_copy(0).wait_recv()
    for z in range(secs):
        k = 2 * secs + z
        edge = jnp.where(t == 1, stiff[1, z] * erecv[0, k : k + 1, :], 0.0)
        for h in range(chunks):
            if h == 0:
                above = jnp.where(row_at == 0, edge, pltpu.roll(vc[z, rows_at(h)], 1, 0))
            else:
                above = vc[z, pl.ds(h * HALF - 1, HALF)]
            va[z, rows_at(h)] = above
            diag[z, rows_at(h)] = diag[z, rows_at(h)] + vc[z, rows_at(h)] + above
    loads[5].wait()

    def reduce_start():
        quarter = LANES // 4
        group = lax.broadcasted_iota(jnp.int32, (1, LANES), 1) // quarter
        packed = jnp.zeros((1, LANES), jnp.float32)
        for i in range(4):
            row = jnp.sum(dots[i], axis=0, keepdims=True)
            part = row[:, 0:LANES]
            for c in range(LANES, cols, LANES):
                part = part + row[:, c : c + LANES]
            part = part + pltpu.roll(part, LANES // 2, 1)
            part = part + pltpu.roll(part, quarter, 1)
            packed = jnp.where(group == i, part, packed)
        sall[...] = packed
        for j in range(1, 2 * n):
            pltpu.make_async_remote_copy(
                sall, gath.at[j - 1], gs_sem.at[0], gr_sem.at[0],
                device_id={"gz": lax.rem(g + j // 2, n), "ta": t if j % 2 == 0 else 1 - t},
                device_id_type=MESH,
            ).start()

    everyone = pltpu.make_async_remote_copy(
        gath, gath, gs_sem.at[0], gr_sem.at[0], device_id=other, device_id_type=MESH
    )
    for op in range(OPS):
        reach_step()
        tasks = [functools.partial(own_pairs, op, s, h) for s in range(1, secs) for h in range(chunks)]
        tasks += [functools.partial(own_springs, op, h) for h in range(chunks)]
        share = -(-len(tasks) // len(pieces))
        for i, (d, h) in enumerate(pieces):
            cross(op, d, h)
            for task in tasks[i * share : (i + 1) * share]:
                if task.func is own_springs and op > 0 and task.args[1] == 0:
                    e_copy(op).wait_recv()
                task()
        if op == OPS - 1:
            while pending:
                reach_step()
            reduce_start()
        else:
            reach_step()
        for z, h in pieces:
            finish(op, z, h)
        if op + 1 < OPS:
            send_edges(op + 1)

    everyone.wait_recv()
    total = sall[...]
    for i in range(2 * n - 1):
        total = total + gath[i]
    group = lax.broadcasted_iota(jnp.int32, (1, LANES), 1) // (LANES // 4)
    rr, rm, mm, mq = (
        jnp.sum(jnp.where(group == i, total, 0.0), axis=1, keepdims=True) for i in range(4)
    )
    alpha0 = rr / rm
    rr1 = alpha0 * (alpha0 * mm) - rr
    ratio = rr1 / rr
    one = 1.0 + ratio
    curve = one * one * rm - 2.0 * one * alpha0 * mm + alpha0 * alpha0 * mq
    alpha1 = rr1 / curve
    c1 = alpha0 + alpha1 * one
    c2 = alpha0 * alpha1
    coef[0:1, :] = jnp.broadcast_to(c1, (1, cols))
    coef[1:2, :] = jnp.broadcast_to(c2, (1, cols))

    everyone.wait_send()
    pltpu.make_async_remote_copy(
        esend, erecv, es_sem.at[0], er_sem.at[0], device_id=other, device_id_type=MESH
    ).wait_send()

    @pl.when(has_lower)
    def _():
        pltpu.make_async_remote_copy(
            up, up, vs_sem.at[0], vr_sem.at[0], device_id=lower, device_id_type=MESH
        ).wait_send()

    @pl.when(has_upper)
    def _():
        pltpu.make_async_remote_copy(
            tsend, trecv, ts_sem.at[0], tr_sem.at[0], device_id=upper, device_id_type=MESH
        ).wait_send()


def body(position, gaps, weights, deltas, springs, damping, stiffness):
    secs, rows, cols = damping.shape
    n = lax.axis_size("gz")
    chunks = rows // HALF
    f32, i32 = jnp.float32, jnp.int32
    edge = -(-3 * secs // 8) * 8
    dma = pltpu.SemaphoreType.DMA
    out = pltpu.VMEM(position.shape, f32)
    anyspace = pl.BlockSpec(memory_space=pl.ANY)
    vmem = pl.BlockSpec(memory_space=pltpu.VMEM)
    field = pltpu.VMEM(position.shape, f32)
    plane = pltpu.VMEM(damping.shape, f32)
    exchange = pltpu.VMEM((OPS,) + position.shape, f32)
    r0, m0, q, coef = pl.pallas_call(
        functools.partial(kernel, n),
        out_shape=(out, out, out, pltpu.VMEM((2, cols), f32)),
        in_specs=[anyspace] * 7,
        out_specs=(vmem,) * 4,
        scratch_shapes=[
            pltpu.SMEM(stiffness.shape, f32),
            field,
            exchange, exchange, exchange,
            pltpu.VMEM((OPS, edge, cols), f32),
            pltpu.VMEM((OPS, edge, cols), f32),
            pltpu.VMEM((1, LANES), f32),
            pltpu.VMEM((2 * n - 1, 1, LANES), f32),
            pltpu.VMEM(gaps.shape, f32),
            pltpu.VMEM(weights.shape, f32),
            pltpu.VMEM(deltas.shape, i32),
            pltpu.VMEM(springs.shape, i32),
            plane, plane, plane, plane, plane, plane,
            field,
            pltpu.VMEM((4, HALF, cols), f32),
            dma((7,)),
            dma((1,)), dma((secs * chunks,)), dma((1,)), dma((secs * chunks,)),
            dma((1,)), dma((OPS,)),
            dma((1,)), dma((1,)),
            pltpu.SemaphoreType.REGULAR((max(len(doublings(n)), 1),)),
        ],
        compiler_params=pltpu.CompilerParams(
            collective_id=0, has_side_effects=True, vmem_limit_bytes=VMEM - 3 * 4 * position.size - 2 * 4 * LANES * HALF
        ),
    )(*[pltpu.with_memory_space_constraint(x, pltpu.HBM) for x in (position, gaps, weights, deltas, springs, damping, stiffness)])
    c1, c2 = coef[0], coef[1]
    return c1 * r0 - c2 * m0, r0 - c1 * m0 + c2 * q


def solution(mesh):
    return jax.shard_map(
        body,
        mesh=mesh,
        in_specs=(
            P(None, "gz", "ta", None),
            P(None, None, "gz", "ta", None),
            P(None, "gz", "ta", None),
            P(None, "gz", "ta", None),
            P(None, "gz", "ta", None),
            P("gz", "ta", None),
            P(None, "gz"),
        ),
        out_specs=(P(None, "gz", "ta", None), P(None, "gz", "ta", None)),
        check_vma=False,
    )
```

```python
import functools

import jax
import jax.numpy as jnp
from jax import lax
from jax.experimental import pallas as pl
from jax.experimental.pallas import tpu as pltpu
from jax.sharding import PartitionSpec as P

MESH = pl.DeviceIdType.MESH
PLACES = 9
HALF = 8
OPS = 3
LANES = 128
VMEM = 67043328


def rolled(values, step):
    axis = values.ndim - 1
    return values if step == 0 else pltpu.roll(values, step % values.shape[axis], axis)


def doublings(n):
    reach, out = 1, []
    while reach < n:
        out.append(reach)
        reach *= 2
    return out


def kernel(
    n, pos_h, gaps_h, wei_h, del_h, spr_h, dam_h, stiff_h,
    r0, m0, qbuf, coef,
    stiff, pos, up, tsend, trecv, esend, erecv, sall, gath,
    gaps, wei, dlt, spr, dam, vc, va, hc, hl, diag, accb, dots,
    load_sem, vs_sem, vr_sem, ts_sem, tr_sem, es_sem, er_sem, gs_sem, gr_sem, reach_sem,
):
    g = lax.axis_index("gz")
    t = lax.axis_index("ta")
    secs, rows, cols = dam_h.shape
    chunks = rows // HALF
    other = {"gz": g, "ta": 1 - t}
    lower = {"gz": g - 1, "ta": t}
    upper = {"gz": g + 1, "ta": t}
    has_lower = g > 0
    has_upper = g < n - 1
    fields = [pos, r0, m0]

    loads = [
        pltpu.make_async_copy(pos_h, pos, load_sem.at[0]),
        pltpu.make_async_copy(spr_h, spr, load_sem.at[1]),
        pltpu.make_async_copy(del_h, dlt, load_sem.at[2]),
        pltpu.make_async_copy(wei_h, wei, load_sem.at[3]),
        pltpu.make_async_copy(dam_h, dam, load_sem.at[4]),
        pltpu.make_async_copy(gaps_h, gaps, load_sem.at[5]),
        pltpu.make_async_copy(stiff_h, stiff, load_sem.at[6]),
    ]
    for load in loads:
        load.start()

    barrier = pltpu.get_barrier_semaphore()
    pl.semaphore_signal(barrier, inc=1, device_id=other, device_id_type=MESH)

    @pl.when(has_lower)
    def _():
        pl.semaphore_signal(barrier, inc=1, device_id=lower, device_id_type=MESH)

    @pl.when(has_upper)
    def _():
        pl.semaphore_signal(barrier, inc=1, device_id=upper, device_id_type=MESH)

    @pl.when(jnp.logical_not(has_upper))
    def _():
        up[...] = jnp.zeros_like(up)

    @pl.when(jnp.logical_not(has_lower))
    def _():
        trecv[...] = jnp.zeros_like(trecv)

    esend[...] = jnp.zeros_like(esend)
    dots[...] = jnp.zeros_like(dots)

    def rows_at(h):
        return pl.ds(h * HALF, HALF)

    def v_copy(op, d, h):
        return pltpu.make_async_remote_copy(
            fields[op].at[:, d, rows_at(h)], up.at[op, :, d, rows_at(h)],
            vs_sem.at[0], vr_sem.at[d * chunks + h], device_id=lower, device_id_type=MESH,
        )

    def t_copy(op, d, h):
        return pltpu.make_async_remote_copy(
            tsend.at[op, :, d, rows_at(h)], trecv.at[op, :, d, rows_at(h)],
            ts_sem.at[0], tr_sem.at[d * chunks + h], device_id=upper, device_id_type=MESH,
        )

    def e_copy(op):
        return pltpu.make_async_remote_copy(
            esend.at[op], erecv.at[op], es_sem.at[0], er_sem.at[op],
            device_id=other, device_id_type=MESH,
        )

    far = doublings(n)

    def reach_signal(i):
        for sign in (-1, 1):
            there = g + sign * far[i]

            @pl.when((there >= 0) & (there < n))
            def _():
                pl.semaphore_signal(
                    reach_sem.at[i], inc=1, device_id={"gz": there, "ta": t}, device_id_type=MESH
                )

    def reach_wait(i):
        pl.semaphore_wait(
            reach_sem.at[i],
            (g >= far[i]).astype(jnp.int32) + (g + far[i] < n).astype(jnp.int32),
        )

    pending = list(range(len(far)))

    def reach_step():
        if pending:
            i = pending.pop(0)
            reach_wait(i)
            if i + 1 < len(far):
                reach_signal(i + 1)

    def send_edges(op):
        for comp in range(2):
            for z in range(secs):
                k = comp * secs + z
                top = fields[op][comp, z, 0:1, :]
                bottom = fields[op][comp, z, rows - 1 : rows, :]
                esend[op, k : k + 1, :] = jnp.where(t == 0, bottom, top)
        if op == 0:
            for z in range(secs):
                k = 2 * secs + z
                esend[op, k : k + 1, :] = jnp.where(
                    spr[1, z, rows - 1 : rows, :] > 0, 1.0, 0.0
                ).astype(jnp.float32)
        e_copy(op).start()

    shape = (HALF, cols)
    columns_at = lax.broadcasted_iota(jnp.int32, shape, 1)
    row_at = lax.broadcasted_iota(jnp.int32, shape, 0)

    def dot_into(i, a, b):
        dots[i] = dots[i] + (a[0] * b[0] + a[1] * b[1])

    def pulls(op, s, h):
        field = fields[op][:, s, rows_at(h)] if s < secs else up[op, :, s - secs, rows_at(h)]
        sources = [(s - k - 1, k) for k in range(3) if 0 <= s - k - 1 < secs]
        got = [None] * len(sources)
        for place in range(PLACES):
            moved = rolled(field, 4 - place)
            for i, (z, k) in enumerate(sources):
                if got[i] is None:
                    got[i] = moved
                else:
                    got[i] = jnp.where((dlt[k, z, rows_at(h)] == place)[None], moved, got[i])
        out = []
        for i, (z, k) in enumerate(sources):
            miss = fields[op][:, z, rows_at(h)] - got[i]
            if op == 0:
                miss = miss - gaps[:, k, z, rows_at(h)]
            out.append((z, k, got[i], miss, wei[k, z, rows_at(h)][None] * miss))
        return out

    def scatter(terms, h):
        total = None
        for place in range(PLACES):
            part = None
            for z, k, _, _, pulled in terms:
                one = jnp.where((dlt[k, z, rows_at(h)] == place)[None], pulled, 0.0)
                part = one if part is None else part + one
            part = rolled(part, place - 4)
            total = part if total is None else total + part
        return total

    def own_pairs(op, s, h):
        here = rows_at(h)
        terms = pulls(op, s, h)
        for z, _, _, _, pulled in terms:
            accb[:, z, here] = accb[:, z, here] + pulled
        accb[:, s, here] = accb[:, s, here] - scatter(terms, h)

    def own_springs(op, h):
        here = rows_at(h)
        for z in range(secs):
            for comp in range(2):
                k = comp * secs + z
                center = fields[op][comp, z, here]
                if h == 0:
                    above = jnp.where(row_at == 0, erecv[op, k : k + 1, :], pltpu.roll(center, 1, 0))
                else:
                    above = fields[op][comp, z, pl.ds(h * HALF - 1, HALF)]
                if h == chunks - 1:
                    below = jnp.where(
                        row_at == HALF - 1, erecv[op, k : k + 1, :], pltpu.roll(center, HALF - 1, 0)
                    )
                else:
                    below = fields[op][comp, z, pl.ds(h * HALF + 1, HALF)]
                accb[comp, z, here] = (
                    accb[comp, z, here]
                    + diag[z, here] * center
                    - hc[z, here] * rolled(center, -1)
                    - hl[z, here] * rolled(center, 1)
                    - vc[z, here] * below
                    - va[z, here] * above
                )
            if op == OPS - 1:
                dot_into(3, fields[op][:, z, here], accb[:, z, here])

    def cross(op, d, h):
        @pl.when(has_upper)
        def _():
            v_copy(op, d, h).wait_recv()

        terms = pulls(op, secs + d, h)
        tsend[op, :, d, rows_at(h)] = scatter(terms, h)

        if op < OPS - 1:
            @pl.when(has_upper)
            def _():
                t_copy(op, d, h).start()

        started = d == 0
        for z, _, partner, _, pulled in terms:
            before = 0.0 if started else accb[:, z, rows_at(h)]
            accb[:, z, rows_at(h)] = before + pulled
            if op == OPS - 1:
                dot_into(3, -partner, pulled)

    def finish(op, z, h):
        here = rows_at(h)

        @pl.when(has_lower)
        def _():
            t_copy(op, z, h).wait_recv()

        image = accb[:, z, here] - trecv[op, :, z, here]
        if op == 0:
            r0[:, z, here] = -image
        elif op == 1:
            m0[:, z, here] = image
        else:
            qbuf[:, z, here] = image
        if op + 1 < OPS:
            @pl.when(has_lower)
            def _():
                v_copy(op + 1, z, h).start()
        if op == 0:
            dot_into(0, image, image)
        elif op == 1:
            dot_into(1, r0[:, z, here], image)
            dot_into(2, image, image)

    pieces = [(d, h) for d in range(secs) for h in range(chunks)]

    held = pieces

    loads[0].wait()
    pl.semaphore_wait(barrier, 1 + has_lower.astype(jnp.int32) + has_upper.astype(jnp.int32))

    @pl.when(has_lower)
    def _():
        for d, h in pieces:
            v_copy(0, d, h).start()

    loads[1].wait()
    send_edges(0)
    if far:
        reach_signal(0)
    loads[2].wait()
    loads[3].wait()
    for k in range(3):
        for z in range(secs):
            inside = jnp.where(g * secs + z + k + 1 < n * secs, 1.0, 0.0).astype(jnp.float32)
            for h in range(chunks):
                target = columns_at + dlt[k, z, rows_at(h)] - 4
                valid = (target >= 0) & (target < cols)
                wei[k, z, rows_at(h)] = jnp.where(valid, wei[k, z, rows_at(h)], 0.0) * inside
    loads[4].wait()
    loads[6].wait()
    for z in range(secs):
        for h in range(chunks):
            last = jnp.where((t == 1) & (row_at == HALF - 1), 0.0, 1.0) if h == chunks - 1 else 1.0
            vc[z, rows_at(h)] = (
                stiff[1, z] * jnp.where(spr[1, z, rows_at(h)] > 0, 1.0, 0.0).astype(jnp.float32) * last
            )
            right = stiff[0, z] * jnp.where(
                (spr[0, z, rows_at(h)] > 0) & (columns_at < cols - 1), 1.0, 0.0
            ).astype(jnp.float32)
            hc[z, rows_at(h)] = right
            left = rolled(right, 1)
            hl[z, rows_at(h)] = left
            diag[z, rows_at(h)] = dam[z, rows_at(h)] + right + left
    e_copy(0).wait_recv()
    for z in range(secs):
        k = 2 * secs + z
        edge = jnp.where(t == 1, stiff[1, z] * erecv[0, k : k + 1, :], 0.0)
        for h in range(chunks):
            if h == 0:
                above = jnp.where(row_at == 0, edge, pltpu.roll(vc[z, rows_at(h)], 1, 0))
            else:
                above = vc[z, pl.ds(h * HALF - 1, HALF)]
            va[z, rows_at(h)] = above
            diag[z, rows_at(h)] = diag[z, rows_at(h)] + vc[z, rows_at(h)] + above
    loads[5].wait()

    quarter = LANES // 4
    group = lax.broadcasted_iota(jnp.int32, (1, LANES), 1) // quarter

    def folded(i):
        row = jnp.sum(dots[i], axis=0, keepdims=True)
        part = row[:, 0:LANES]
        for c in range(LANES, cols, LANES):
            part = part + row[:, c : c + LANES]
        part = part + pltpu.roll(part, LANES // 2, 1)
        return part + pltpu.roll(part, quarter, 1)

    def pack_known():
        packed = jnp.zeros((1, LANES), jnp.float32)
        for i in range(OPS):
            packed = jnp.where(group == i, folded(i), packed)
        sall[...] = packed

    def reduce_start():
        part = folded(OPS)
        sall[...] = jnp.where(group == OPS, part, sall[...])
        for j in range(1, 2 * n):
            pltpu.make_async_remote_copy(
                sall, gath.at[j - 1], gs_sem.at[0], gr_sem.at[0],
                device_id={"gz": lax.rem(g + j // 2, n), "ta": t if j % 2 == 0 else 1 - t},
                device_id_type=MESH,
            ).start()

    everyone = pltpu.make_async_remote_copy(
        gath, gath, gs_sem.at[0], gr_sem.at[0], device_id=other, device_id_type=MESH
    )
    for op in range(OPS):
        reach_step()
        tasks = [functools.partial(own_pairs, op, s, h) for s in range(1, secs) for h in range(chunks)]
        tasks += [functools.partial(own_springs, op, h) for h in range(chunks)]
        share = -(-len(tasks) // len(pieces))
        for i, (d, h) in enumerate(pieces):
            cross(op, d, h)
            for task in tasks[i * share : (i + 1) * share]:
                if task.func is own_springs and op > 0 and task.args[1] == 0:
                    e_copy(op).wait_recv()
                task()
        if op == OPS - 1:
            while pending:
                reach_step()
            reduce_start()

            @pl.when(has_upper)
            def _():
                for d, h in held:
                    t_copy(op, d, h).start()
        else:
            reach_step()
        for z, h in pieces:
            finish(op, z, h)
        if op + 1 < OPS:
            send_edges(op + 1)
        if op == OPS - 2:
            pack_known()

    everyone.wait_recv()
    total = sall[...]
    for i in range(2 * n - 1):
        total = total + gath[i]
    rr, rm, mm, mq = (
        jnp.sum(jnp.where(group == i, total, 0.0), axis=1, keepdims=True) for i in range(4)
    )
    alpha0 = rr / rm
    rr1 = alpha0 * (alpha0 * mm) - rr
    ratio = rr1 / rr
    one = 1.0 + ratio
    curve = one * one * rm - 2.0 * one * alpha0 * mm + alpha0 * alpha0 * mq
    alpha1 = rr1 / curve
    c1 = alpha0 + alpha1 * one
    c2 = alpha0 * alpha1
    coef[0:1, :] = jnp.broadcast_to(c1, (1, cols))
    coef[1:2, :] = jnp.broadcast_to(c2, (1, cols))

    everyone.wait_send()
    pltpu.make_async_remote_copy(
        esend, erecv, es_sem.at[0], er_sem.at[0], device_id=other, device_id_type=MESH
    ).wait_send()

    @pl.when(has_lower)
    def _():
        pltpu.make_async_remote_copy(
            up, up, vs_sem.at[0], vr_sem.at[0], device_id=lower, device_id_type=MESH
        ).wait_send()

    @pl.when(has_upper)
    def _():
        pltpu.make_async_remote_copy(
            tsend, trecv, ts_sem.at[0], tr_sem.at[0], device_id=upper, device_id_type=MESH
        ).wait_send()


def body(position, gaps, weights, deltas, springs, damping, stiffness):
    secs, rows, cols = damping.shape
    n = lax.axis_size("gz")
    chunks = rows // HALF
    f32, i32 = jnp.float32, jnp.int32
    edge = -(-3 * secs // 8) * 8
    dma = pltpu.SemaphoreType.DMA
    out = pltpu.VMEM(position.shape, f32)
    anyspace = pl.BlockSpec(memory_space=pl.ANY)
    vmem = pl.BlockSpec(memory_space=pltpu.VMEM)
    field = pltpu.VMEM(position.shape, f32)
    plane = pltpu.VMEM(damping.shape, f32)
    exchange = pltpu.VMEM((OPS,) + position.shape, f32)
    r0, m0, q, coef = pl.pallas_call(
        functools.partial(kernel, n),
        out_shape=(out, out, out, pltpu.VMEM((2, cols), f32)),
        in_specs=[anyspace] * 7,
        out_specs=(vmem,) * 4,
        scratch_shapes=[
            pltpu.SMEM(stiffness.shape, f32),
            field,
            exchange, exchange, exchange,
            pltpu.VMEM((OPS, edge, cols), f32),
            pltpu.VMEM((OPS, edge, cols), f32),
            pltpu.VMEM((1, LANES), f32),
            pltpu.VMEM((2 * n - 1, 1, LANES), f32),
            pltpu.VMEM(gaps.shape, f32),
            pltpu.VMEM(weights.shape, f32),
            pltpu.VMEM(deltas.shape, i32),
            pltpu.VMEM(springs.shape, i32),
            plane, plane, plane, plane, plane, plane,
            field,
            pltpu.VMEM((4, HALF, cols), f32),
            dma((7,)),
            dma((1,)), dma((secs * chunks,)), dma((1,)), dma((secs * chunks,)),
            dma((1,)), dma((OPS,)),
            dma((1,)), dma((1,)),
            pltpu.SemaphoreType.REGULAR((max(len(doublings(n)), 1),)),
        ],
        compiler_params=pltpu.CompilerParams(
            collective_id=0, has_side_effects=True, vmem_limit_bytes=VMEM - 3 * 4 * position.size - 2 * 4 * LANES * HALF
        ),
    )(*[pltpu.with_memory_space_constraint(x, pltpu.HBM) for x in (position, gaps, weights, deltas, springs, damping, stiffness)])
    c1, c2 = coef[0], coef[1]
    return c1 * r0 - c2 * m0, r0 - c1 * m0 + c2 * q


def solution(mesh):
    return jax.shard_map(
        body,
        mesh=mesh,
        in_specs=(
            P(None, "gz", "ta", None),
            P(None, None, "gz", "ta", None),
            P(None, "gz", "ta", None),
            P(None, "gz", "ta", None),
            P(None, "gz", "ta", None),
            P("gz", "ta", None),
            P(None, "gz"),
        ),
        out_specs=(P(None, "gz", "ta", None), P(None, "gz", "ta", None)),
        check_vma=False,
    )
```
